32 devices in a mesh: section: 2 (over core), dp: 16 (over z, y, x).
Axes of the slice: x: 2, y: 2, z: 4, core: 2. Of those that a mesh axis runs over, the one named last changes fastest.
Arguments:
- tokens: bfloat16 [2, 16, 80, 1024], P(None, 'dp'), may hold values from -6 to 6
- w_qkv: bfloat16 [2, 1024, 1536], P('section', 'dp'), may hold values from -0.1875 to 0.1875
- w_output: bfloat16 [2, 512, 1024], P('section', None, 'dp'), may hold values from -0.25 to 0.25
- tangent_value: bfloat16 [2, 2, 1024, 512], P('section', None, 'dp'), may hold values from -0.1875 to 0.1875
- tangent_output: bfloat16 [2, 2, 512, 1024], P('section', None, None, 'dp'), may hold values from -0.25 to 0.25
- layer_gain: float32 [2, 1024], P('section'), may hold values from 0.5 to 1.5
- final_gain: float32 [1024], replicated, may hold values from 0.5 to 1.5
- head: bfloat16 [1024, 1000], P(None, 'section'), may hold values from -0.1875 to 0.1875
Outputs:
- mean_logits: float32 [2, 16, 1000], P(None, 'dp', 'section')
- variance: float32 [2, 16, 1000], P(None, 'dp', 'section')
The draws below stay inside these ranges and needn't reach their ends.
All inputs are finite; a program needn't handle non-finite values.
Results may differ from the reference program's by a relative error of at most 0.018.
Values may be sent and summed in bfloat16 or wider, within the bound.
A program may use at most 64 MiB of HBM per device.

```python
import jax
import jax.numpy as jnp
from jax import lax

D = 1024
HEADS = 8
HEAD = 64
CLASSES = 1000
TOK = 80
TANGENTS = 2
MICRO = 2
HD = 512
IMAGES = 16
SECTIONS = 2
N_SECTION = 2


def level_of(rng, extent, cuts, least, largest):
    def one(dim, shards_of):
        draws = jax.random.uniform(jax.random.fold_in(jax.random.fold_in(rng, 6), dim), (shards_of,), jnp.float32, least / len(cuts), largest / len(cuts))
        return jnp.repeat(jnp.exp(draws), extent[dim] // shards_of).reshape((-1,) + (1,) * (len(extent) - dim - 1))

    factor_of = one(*cuts[0])
    for cut in cuts[1:]:
        factor_of = factor_of * one(*cut)
    return factor_of


def bell_draw(stream_key, extent, spread, reach, split=(), held_as=jnp.bfloat16):
    result = jax.random.normal(stream_key, extent, jnp.float32) * spread
    if len(split) > 0:
        result = level_of(stream_key, extent, split, -0.22, 0.18) * result
    return jnp.clip(result, min=-reach, max=reach).astype(held_as)


def setup_inputs(seed: int = 0) -> dict:
    key_of = jax.random.split(jax.random.key(seed), 9)
    tokens = bell_draw(key_of[0], (MICRO, IMAGES, TOK, D), 1.0, 6.0, ((1, 16),))
    w_qkv = bell_draw(key_of[1], (SECTIONS, D, 3 * HD), D ** -0.5, 0.1875, ((0, 2), (1, 16)))
    w_output = bell_draw(key_of[2], (SECTIONS, HD, D), HD ** -0.5, 0.25, ((0, 2), (2, 16)))
    tangent_value = bell_draw(key_of[3], (SECTIONS, TANGENTS, D, HD), D ** -0.5, 0.1875, ((0, 2), (2, 16)))
    tangent_output = bell_draw(key_of[4], (SECTIONS, TANGENTS, HD, D), HD ** -0.5, 0.25, ((0, 2), (3, 16)))
    layer_gain = jnp.clip(1.0 + 0.1 * jax.random.normal(key_of[5], (SECTIONS, D), jnp.float32), 0.5, 1.5)
    final_gain = jnp.clip(1.0 + 0.1 * jax.random.normal(key_of[6], (D,), jnp.float32), 0.5, 1.5)
    head = bell_draw(key_of[7], (D, CLASSES), D ** -0.5, 0.1875, ((1, 2),))
    return {"tokens": tokens, "w_qkv": w_qkv, "w_output": w_output, "tangent_value": tangent_value, "tangent_output": tangent_output, "layer_gain": layer_gain, "final_gain": final_gain, "head": head}


epsilon = 1e-06

def widen(array):
    return array.astype(jnp.float32)

def norm_jvp(primal, tangents, gains):
    average = lax.optimization_barrier(jnp.mean(primal, -1, keepdims=True))
    centred = primal - average
    inverse = lax.rsqrt(lax.optimization_barrier(jnp.mean(centred * centred, -1, keepdims=True)) + epsilon)
    dcentred = tangents - lax.optimization_barrier(jnp.mean(tangents, -1, keepdims=True))
    dinverse = -inverse ** 3 * lax.optimization_barrier(jnp.mean(centred * dcentred, -1, keepdims=True))
    return (centred * inverse * gains, (dcentred * inverse + centred * dinverse) * gains)

def layer_step(state, qkv_weight, out_weight, value_tangent, out_tangent, gains):
    resid = widen(state)
    normed_zero, normed_rest = norm_jvp(resid[0], resid[1:], gains)
    normed = jnp.concatenate([normed_zero[None], normed_rest]).astype(jnp.bfloat16)
    streams, batch, tokens_here, width = normed.shape
    projected = jnp.einsum('sbtd,de->sbte', widen(normed), widen(qkv_weight))
    extra_value = jnp.einsum('btd,kde->kbte', widen(normed[0]), widen(value_tangent))
    queries = projected[..., :HD]
    key_rows = projected[..., HD:2 * HD]
    values = projected[..., 2 * HD:]
    values = jnp.concatenate([values[:1], values[1:] + extra_value])
    shape_heads = (streams, batch, tokens_here, HEADS, HEAD)
    queries = queries.astype(jnp.bfloat16).reshape(shape_heads)
    key_rows = key_rows.astype(jnp.bfloat16).reshape(shape_heads)
    values = values.astype(jnp.bfloat16).reshape(shape_heads)
    factor = HEAD ** (-0.5)
    scores = jnp.einsum('bqhe,bkhe->bhqk', widen(queries[0]), widen(key_rows[0])) * factor
    probs = jax.nn.softmax(scores, -1)
    dscores = (jnp.einsum('sbqhe,bkhe->sbhqk', widen(queries[1:]), widen(key_rows[0])) + jnp.einsum('bqhe,sbkhe->sbhqk', widen(queries[0]), widen(key_rows[1:]))) * factor
    dprobs = probs * (dscores - lax.optimization_barrier(jnp.sum(probs * dscores, -1, keepdims=True)))
    probs_low = probs.astype(jnp.bfloat16)
    dprobs_low = dprobs.astype(jnp.bfloat16)
    attended_zero = jnp.einsum('bhqk,bkhe->bqhe', widen(probs_low), widen(values[0]))
    attended_rest = jnp.einsum('sbhqk,bkhe->sbqhe', widen(dprobs_low), widen(values[0])) + jnp.einsum('bhqk,sbkhe->sbqhe', widen(probs_low), widen(values[1:]))
    attended = jnp.concatenate([attended_zero[None], attended_rest]).astype(jnp.bfloat16)
    attended = attended.reshape(streams, batch, tokens_here, HD)
    output = jnp.einsum('sbte,ed->sbtd', widen(attended), widen(out_weight))
    extra_out = jnp.einsum('bte,ked->kbtd', widen(attended[0]), widen(out_tangent))
    output = jnp.concatenate([output[:1], output[1:] + extra_out])
    return (resid + output).astype(jnp.bfloat16)

def reference(tokens, w_qkv, w_output, tangent_value, tangent_output, layer_gain, final_gain, head):
    micro_count, image_count = (tokens.shape[0], tokens.shape[1])
    flat = tokens.reshape(micro_count * image_count, TOK, D)
    state = jnp.concatenate([flat[None], jnp.zeros((TANGENTS, micro_count * image_count, TOK, D), jnp.bfloat16)])
    for layer in range(N_SECTION):
        state = layer_step(state, w_qkv[layer], w_output[layer], tangent_value[layer], tangent_output[layer], layer_gain[layer])
    class_rows = widen(state[:, :, 0, :])
    final_zero, final_rest = norm_jvp(class_rows[0], class_rows[1:], final_gain)
    normed_final = jnp.concatenate([final_zero[None], final_rest]).astype(jnp.bfloat16)
    logits = jnp.einsum('sbd,dc->sbc', widen(normed_final), widen(head))
    mean_logits = logits[0].reshape(micro_count, image_count, CLASSES)
    variance = lax.optimization_barrier(jnp.sum(logits[1:] * logits[1:], 0)).reshape(micro_count, image_count, CLASSES)
    return (mean_logits, variance)
```

```python
import functools

import jax
import jax.numpy as jnp
from jax import lax
from jax.experimental import pallas as pl
from jax.experimental.pallas import tpu as pltpu
from jax.sharding import PartitionSpec as P

HEAD = 64
epsilon = 1e-06
F32, BF16 = jnp.float32, jnp.bfloat16
MESH = pl.DeviceIdType.MESH


def contract(spec, left, right):
    return jnp.einsum(spec, left, right, preferred_element_type=jnp.float32)


def norm_jvp(primal, tangents, gains):
    average = jnp.mean(primal, -1, keepdims=True)
    centred = primal - average
    inverse = lax.rsqrt(jnp.mean(centred * centred, -1, keepdims=True) + epsilon)
    dcentred = tangents - jnp.mean(tangents, -1, keepdims=True)
    dinverse = -(inverse**3) * jnp.mean(centred * dcentred, -1, keepdims=True)
    return (centred * inverse * gains, (dcentred * inverse + centred * dinverse) * gains)


def layer_step(state, qkv_weight, out_weight, value_tangent, out_tangent, gains):
    hd = out_weight.shape[0]
    heads = hd // HEAD
    resid = state.astype(F32)
    normed_zero, normed_rest = norm_jvp(resid[0], resid[1:], gains)
    normed = jnp.concatenate([normed_zero[None], normed_rest]).astype(BF16)
    streams, batch, tokens_here, width = normed.shape
    projected = contract("sbtd,de->sbte", normed, qkv_weight)
    extra_value = contract("btd,kde->kbte", normed[0], value_tangent)
    queries = projected[..., :hd]
    key_rows = projected[..., hd : 2 * hd]
    values = projected[..., 2 * hd :]
    values = jnp.concatenate([values[:1], values[1:] + extra_value])
    shape_heads = (streams, batch, tokens_here, heads, HEAD)
    queries = queries.astype(BF16).reshape(shape_heads)
    key_rows = key_rows.astype(BF16).reshape(shape_heads)
    values = values.astype(BF16).reshape(shape_heads)
    factor = HEAD ** (-0.5)
    scores = contract("bqhe,bkhe->bhqk", queries[0], key_rows[0]) * factor
    probs = jax.nn.softmax(scores, -1)
    dscores = (
        contract("sbqhe,bkhe->sbhqk", queries[1:], key_rows[0])
        + contract("bqhe,sbkhe->sbhqk", queries[0], key_rows[1:])
    ) * factor
    dprobs = probs * (dscores - jnp.sum(probs * dscores, -1, keepdims=True))
    probs_low = probs.astype(BF16)
    dprobs_low = dprobs.astype(BF16)
    attended_zero = contract("bhqk,bkhe->bqhe", probs_low, values[0])
    attended_rest = contract("sbhqk,bkhe->sbqhe", dprobs_low, values[0]) + contract(
        "bhqk,sbkhe->sbqhe", probs_low, values[1:]
    )
    attended = jnp.concatenate([attended_zero[None], attended_rest]).astype(BF16)
    attended = attended.reshape(streams, batch, tokens_here, hd)
    output = contract("sbte,ed->sbtd", attended, out_weight)
    extra_out = contract("bte,ked->kbtd", attended[0], out_tangent)
    output = jnp.concatenate([output[:1], output[1:] + extra_out])
    return (resid + output).astype(BF16)


def relay_shards(tokens, w_qkv, w_output, tangent_value, tangent_output, layer_gain, final_gain, head):
    full_qkv, full_output, full_value_tan, full_output_tan = (
        lax.all_gather(w_qkv, "dp", axis=1, tiled=True),
        lax.all_gather(w_output, "dp", axis=2, tiled=True),
        lax.all_gather(tangent_value, "dp", axis=2, tiled=True),
        lax.all_gather(tangent_output, "dp", axis=3, tiled=True),
    )
    tangents = tangent_value.shape[1]

    def advance_layer(state):
        return layer_step(
            state, full_qkv[0], full_output[0], full_value_tan[0], full_output_tan[0], layer_gain[0]
        )

    section_index = lax.axis_index("section")
    section_count = lax.axis_size("section")
    route = [(i, i + 1) for i in range(section_count - 1)]
    micro, _, toks, width = tokens.shape
    entering = jnp.concatenate(
        [tokens.reshape(1, micro, toks, width), jnp.zeros((tangents, micro, toks, width), BF16)]
    )

    def advance(step, outgoing):
        incoming = lax.ppermute(outgoing, "section", route)
        source = jnp.where(step == 0, entering, incoming)
        return lax.cond(section_index == step, advance_layer, jnp.zeros_like, source)

    finished = lax.fori_loop(0, section_count, advance, jnp.zeros_like(entering))
    collected = finished[:, :, 0, :]
    mine = section_index == section_count - 1
    features = lax.psum(jnp.where(mine, collected, jnp.zeros_like(collected)), "section")
    widened = features.astype(F32)
    final_zero, final_rest = norm_jvp(widened[0], widened[1:], final_gain)
    normed_final = jnp.concatenate([final_zero[None], final_rest]).astype(BF16)
    logits = contract("sbd,dc->sbc", normed_final, head)
    return (logits[0][:, None, :], jnp.sum(logits[1:] * logits[1:], 0)[:, None, :])


def dot(a, b):
    return lax.dot_general(a, b, (((1,), (0,)), ((), ())), preferred_element_type=F32)


def dot_t(a, b):
    return lax.dot_general(a, b, (((1,), (1,)), ((), ())), preferred_element_type=F32)


class Gather:
    def __init__(self, n, a_full, b_full, send, recv):
        self.nz = n // 4
        self.a_full, self.b_full, self.send, self.recv = a_full, b_full, send, recv
        self.rows = a_full.shape[0] // n
        self.me = lax.axis_index("dp")
        self.section = lax.axis_index("section")
        me = self.me
        self.x_near = me + 1 - 2 * (me % 2)
        self.y_near = me + 2 - 4 * ((me // 2) % 2)
        self.z = me // 4
        self.diagonal = self.x_near + self.y_near - me
        self.sends = []
        self.slot = 0

    def piece(self, src, group, half):
        depth = self.rows // 2
        at = pl.ds(pl.multiple_of(src * self.rows + half * depth, depth), depth)
        return self.a_full.at[at, :] if group == 0 else self.b_full.at[:, at, :]

    def copy(self, src, group, half, target, slot):
        ref = self.piece(src, group, half)
        return pltpu.make_async_remote_copy(
            src_ref=ref,
            dst_ref=ref,
            send_sem=self.send.at[slot],
            recv_sem=self.recv.at[src, group * 2 + half],
            device_id={"section": self.section, "dp": target},
            device_id_type=MESH,
        )

    def forward(self, cond, src, group, half, target):
        slot = self.slot
        self.slot += 1

        def go():
            self.copy(src, group, half, target, slot).start()

        def end():
            self.copy(src, group, half, target, slot).wait_send()

        if cond is None:
            go()
        else:
            pl.when(cond)(go)
        self.sends.append((cond, end))

    def arrived(self, src, group, half):
        self.copy(src, group, half, self.me, 0).wait_recv()

    def sources(self, d):
        if d == 0:
            return [(0, None)]
        return [(-d, self.z >= d), (d, self.z + d < self.nz)]

    def direct(self, group, d):
        for shift, cond in self.sources(d):
            src = self.me + 4 * shift
            for half in range(2):
                if d > 0:
                    pl.when(cond)(functools.partial(self.arrived, src, group, half))
                if shift <= 0 and d < self.nz - 1:
                    up = self.z + 1 < self.nz
                    self.forward(up if cond is None else cond & up, src, group, half, self.me + 4)
                if shift >= 0 and d < self.nz - 1:
                    down = self.z >= 1
                    self.forward(down if cond is None else cond & down, src, group, half, self.me - 4)
                order = ((self.y_near, self.x_near), (self.x_near, self.y_near))[half]
                for target in order:
                    self.forward(cond, src, group, half, target)

    def relay(self, group, d):
        for shift, cond in self.sources(d):
            for half, near, target in ((0, self.x_near, self.y_near), (1, self.y_near, self.x_near)):
                src = near + 4 * shift
                wait = functools.partial(self.arrived, src, group, half)
                wait() if cond is None else pl.when(cond)(wait)
                self.forward(cond, src, group, half, target)

    def rest(self, group):
        for z in range(self.nz):
            up = 4 * (z - self.z)
            self.arrived(self.x_near + up, group, 1)
            self.arrived(self.y_near + up, group, 0)
            self.arrived(self.diagonal + up, group, 0)
            self.arrived(self.diagonal + up, group, 1)

    def drain(self):
        for cond, end in self.sends:
            end() if cond is None else pl.when(cond)(end)
        self.sends = []


def send_slots(n):
    nz = n // 4
    return 2 * 2 * (4 + 3 * 2 * (nz - 1) + 2 * nz)


def norm_rows(x, gains):
    average = jnp.mean(x, -1, keepdims=True)
    centred = x - average
    inverse = lax.rsqrt(jnp.mean(centred * centred, -1, keepdims=True) + epsilon)
    return centred, inverse, centred * inverse * gains


def norm_tangent(t, centred, inverse, gains):
    dcentred = t - jnp.mean(t, -1, keepdims=True)
    dinverse = -(inverse * inverse * inverse) * jnp.mean(centred * dcentred, -1, keepdims=True)
    return (dcentred * inverse + centred * dinverse) * gains


def softmax(scores):
    e = jnp.exp(scores - jnp.max(scores, -1, keepdims=True))
    return e / jnp.sum(e, -1, keepdims=True)


def first_layer(sizes, tokens, gain, a_full, b_full, normed, proj, att, state):
    micro, toks, width, hd, tangents = sizes
    for b in range(micro):
        x = tokens[b].astype(F32)
        normed[0, pl.ds(b * toks, toks), :] = norm_rows(x, gain[...])[2].astype(BF16)
    n = normed[0]
    for c in range(3 + tangents):
        at = pl.ds(c * hd, hd)
        proj[:, at] = dot(n, a_full[:, at]).astype(BF16)
    factor = HEAD ** (-0.5)
    even = lax.broadcasted_iota(jnp.int32, (toks, 2 * HEAD), 1) < HEAD
    even_v = lax.broadcasted_iota(jnp.int32, (toks, 2 * HEAD), 1) < HEAD
    for b in range(micro):
        rows = pl.ds(b * toks, toks)
        for pair in range(hd // (2 * HEAD)):
            lanes = pair * 2 * HEAD
            q = proj[rows, pl.ds(lanes, 2 * HEAD)]
            k = proj[rows, pl.ds(hd + lanes, 2 * HEAD)]
            vs = [proj[rows, pl.ds((2 + s) * hd + lanes, 2 * HEAD)] for s in range(1 + tangents)]
            zero = jnp.zeros_like(q)
            low = []
            for mine in (jnp.where(even, q, zero), jnp.where(even, zero, q)):
                low.append(softmax(dot_t(mine, k) * factor).astype(BF16))
            for s, v in enumerate(vs):
                joined = jnp.where(even_v, dot(low[0], v), dot(low[1], v))
                att[pl.ds(s * micro * toks + b * toks, toks), pl.ds(lanes, 2 * HEAD)] = joined.astype(BF16)
    rows0 = micro * toks
    tile = 256
    for c in range(width // tile):
        at = pl.ds(c * tile, tile)
        out = dot_t(att[...], b_full[0, at, :])
        extra = [dot_t(att[pl.ds(0, rows0), :], b_full[1 + j, at, :]) for j in range(tangents)]
        for b in range(micro):
            x = tokens[b, :, at].astype(F32)
            state[pl.ds(b * toks, toks), at] = (x + out[b * toks : (b + 1) * toks]).astype(BF16)
        for j in range(tangents):
            state[pl.ds((1 + j) * rows0, rows0), at] = (
                out[(1 + j) * rows0 : (2 + j) * rows0] + extra[j]
            ).astype(BF16)


def last_layer(sizes, gain, a_full, b_full, normed, state, classes):
    micro, toks, width, hd, tangents = sizes
    streams = 1 + tangents
    heads = hd // HEAD
    rows0 = micro * toks
    for b in range(micro):
        at = pl.ds(b * toks, toks)
        centred, inverse, y = norm_rows(state[at, :].astype(F32), gain[...])
        normed[0, at, :] = y.astype(BF16)
        for j in range(tangents):
            t = state[pl.ds((1 + j) * rows0 + b * toks, toks), :].astype(F32)
            normed[1 + j, at, :] = norm_tangent(t, centred, inverse, gain[...]).astype(BF16)
    block = 16
    firsts = [normed[s, pl.ds(b * toks, block), :] for b in range(micro) for s in range(streams)]
    q = dot(jnp.concatenate(firsts, 0), a_full[:, pl.ds(0, hd)])
    q = q.astype(BF16).astype(F32)
    mask = (
        lax.broadcasted_iota(jnp.int32, (heads, hd), 1) // HEAD
        == lax.broadcasted_iota(jnp.int32, (heads, hd), 0)
    ).astype(F32)
    spread = [q[i * block : i * block + 1] * mask for i in range(micro * streams)]
    u = dot_t(jnp.concatenate(spread, 0).astype(BF16), a_full[:, pl.ds(hd, hd)])
    factor = HEAD ** (-0.5)
    sums = []
    for b in range(micro):
        at = pl.ds(b * toks, toks)
        ub = u[b * streams * heads : (b + 1) * streams * heads]
        base = dot_t(ub.astype(BF16), normed[0, at, :]) * factor
        u0 = ub[:heads].astype(BF16)
        probs = softmax(base[:heads])
        weights = [probs]
        for j in range(tangents):
            ds = base[(1 + j) * heads : (2 + j) * heads] + dot_t(u0, normed[1 + j, at, :]) * factor
            weights.append(probs * (ds - jnp.sum(probs * ds, -1, keepdims=True)))
        m = dot(jnp.concatenate(weights, 0).astype(BF16), normed[0, at, :])
        low = probs.astype(BF16)
        parts = [m[:heads]]
        for j in range(tangents):
            parts.append(m[(1 + j) * heads : (2 + j) * heads] + dot(low, normed[1 + j, at, :]))
        sums += parts
    stacked = jnp.concatenate(sums, 0).astype(BF16)
    r = dot(stacked, a_full[:, pl.ds(2 * hd, hd)])
    zeros = jnp.concatenate([sums[b * streams] for b in range(micro)], 0).astype(BF16)
    extra = [dot(zeros, a_full[:, pl.ds((3 + j) * hd, hd)]) for j in range(tangents)]
    attended = []
    for s in range(streams):
        for b in range(micro):
            i = b * streams + s
            part = r[i * heads : (i + 1) * heads]
            if s > 0:
                part = part + extra[s - 1][b * heads : (b + 1) * heads]
            attended.append(jnp.sum(part * mask, 0, keepdims=True))
    total = classes.shape[0]
    attended.append(jnp.zeros((total - micro * streams, hd), F32))
    low = jnp.concatenate(attended, 0).astype(BF16)
    out = dot_t(low, b_full[0])
    more = [dot_t(low, b_full[1 + j])[:micro] for j in range(tangents)]
    filler = jnp.zeros((total - micro * streams, width), F32)
    out = out + jnp.concatenate([jnp.zeros((micro, width), F32)] + more + [filler], 0)
    resid = [
        state[pl.ds(s * rows0 + b * toks, 16), :].astype(F32)[:1] for s in range(streams) for b in range(micro)
    ]
    resid = jnp.concatenate(resid + [filler], 0)
    classes[...] = (resid + out).astype(BF16).astype(F32)


def kernel(
    n, sizes, tokens, w_qkv, tangent_value, outs, gain, final_gain, head, mean_ref, var_ref,
    a_full, b_full, normed, proj, att, state, state_in, classes, classes_in,
    send, recv, local, gate, core_sems,
):
    micro, toks, width, hd, tangents = sizes
    g = Gather(n, a_full, b_full, send, recv)
    me, section = g.me, g.section
    other = 1 - section
    up, down = g.z + 1 < g.nz, g.z >= 1

    barrier = pltpu.get_barrier_semaphore()

    def greet(target, sec):
        pl.semaphore_signal(
            barrier, inc=1, device_id={"section": sec, "dp": target}, device_id_type=MESH
        )

    greet(g.x_near, section)
    greet(g.y_near, section)
    greet(me, other)
    pl.when(up)(lambda: greet(me + 4, section))
    pl.when(down)(lambda: greet(me - 4, section))

    own = pl.ds(pl.multiple_of(me * g.rows, g.rows), g.rows)
    moves = [pltpu.make_async_copy(w_qkv, a_full.at[own, pl.ds(0, 3 * hd)], local.at[0])]
    for j in range(tangents):
        moves.append(
            pltpu.make_async_copy(
                tangent_value.at[j], a_full.at[own, pl.ds((3 + j) * hd, hd)], local.at[1 + j]
            )
        )
    moves.append(pltpu.make_async_copy(outs, b_full.at[:, own, :], local.at[1 + tangents]))
    for move in moves:
        move.start()
    for move in moves:
        move.wait()
    if g.nz > 1:
        middle = up & down
        pl.when(middle)(lambda: pl.semaphore_wait(barrier, 5))
        pl.when(jnp.logical_not(middle))(lambda: pl.semaphore_wait(barrier, 4))
    else:
        pl.semaphore_wait(barrier, 3)

    pl.when(section == 1)(lambda: pl.semaphore_wait(gate, 1))
    steps = [(group, d) for group in range(2) for d in range(g.nz)]
    g.direct(*steps[0])
    for i, step in enumerate(steps):
        if i + 1 < len(steps):
            g.direct(*steps[i + 1])
        g.relay(*step)
    g.rest(0)
    g.rest(1)
    g.drain()

    def across(src, dst, i):
        return pltpu.make_async_remote_copy(
            src_ref=src,
            dst_ref=dst,
            send_sem=core_sems.at[2 * i],
            recv_sem=core_sems.at[2 * i + 1],
            device_id={"section": other, "dp": me},
            device_id_type=MESH,
        )

    @pl.when(section == 0)
    def _():
        pl.semaphore_signal(
            gate, inc=1, device_id={"section": other, "dp": me}, device_id_type=MESH
        )
        first_layer(sizes, tokens, gain, a_full, b_full, normed, proj, att, state)
        onward = across(state, state_in, 0)
        onward.start()
        onward.wait_send()
        across(classes, classes_in, 1).wait_recv()

    @pl.when(section == 1)
    def _():
        across(state, state_in, 0).wait_recv()
        last_layer(sizes, gain, a_full, b_full, normed, state_in, classes)
        back = across(classes, classes_in, 1)
        back.start()
        classes_in[...] = classes[...]
        back.wait_send()

    rows = classes_in[...]
    count = classes_in.shape[0]
    primal = jnp.concatenate([rows[:micro]] * (1 + tangents) + [rows[(1 + tangents) * micro :]], 0)
    centred, inverse, y = norm_rows(primal, final_gain[...])
    dy = norm_tangent(rows, centred, inverse, final_gain[...])
    which = lax.broadcasted_iota(jnp.int32, (count, width), 0)
    logits = dot(jnp.where(which < micro, y, dy).astype(BF16), head[...])
    mean_ref[...] = logits[:micro]
    var_ref[...] = sum(
        logits[(1 + j) * micro : (2 + j) * micro] * logits[(1 + j) * micro : (2 + j) * micro]
        for j in range(tangents)
    )


def two_sections(n):
    def shards(tokens, w_qkv, w_output, tangent_value, tangent_output, layer_gain, final_gain, head):
        micro, _, toks, width = tokens.shape
        tangents = tangent_value.shape[1]
        hd = w_output.shape[1]
        classes = head.shape[1]
        rows = width // n
        outs = jnp.swapaxes(jnp.concatenate([w_output, tangent_output[0]], 0), 1, 2)
        sizes = (micro, toks, width, hd, tangents)
        vmem = pl.BlockSpec(memory_space=pltpu.VMEM)
        anywhere = pl.BlockSpec(memory_space=pl.ANY)
        streams = 1 + tangents
        padded = -(-micro * streams // 8) * 8
        all_rows = streams * micro * toks
        mean, var = pl.pallas_call(
            functools.partial(kernel, n, sizes),
            out_shape=[jax.ShapeDtypeStruct((micro, classes), F32)] * 2,
            in_specs=[vmem, anywhere, anywhere, anywhere, vmem, vmem, vmem],
            out_specs=[vmem, vmem],
            scratch_shapes=[
                pltpu.VMEM((width, (3 + tangents) * hd), BF16),
                pltpu.VMEM((streams, width, hd), BF16),
                pltpu.VMEM((streams, micro * toks, width), BF16),
                pltpu.VMEM((micro * toks, (3 + tangents) * hd), BF16),
                pltpu.VMEM((all_rows, hd), BF16),
                pltpu.VMEM((all_rows, width), BF16),
                pltpu.VMEM((all_rows, width), BF16),
                pltpu.VMEM((padded, width), F32),
                pltpu.VMEM((padded, width), F32),
                pltpu.SemaphoreType.DMA((send_slots(n),)),
                pltpu.SemaphoreType.DMA((n, 4)),
                pltpu.SemaphoreType.DMA((2 + tangents,)),
                pltpu.SemaphoreType.REGULAR,
                pltpu.SemaphoreType.DMA((4,)),
            ],
            compiler_params=pltpu.CompilerParams(
                collective_id=0, has_side_effects=True, vmem_limit_bytes=60 * 2**20
            ),
        )(
            tokens.reshape(micro, toks, width),
            w_qkv[0],
            tangent_value[0],
            outs,
            layer_gain,
            final_gain[None],
            head,
        )
        return mean[:, None, :], var[:, None, :]

    return shards


def solution(mesh):
    n = mesh.shape["dp"]
    fast = mesh.shape["section"] == 2 and n % 4 == 0
    return jax.shard_map(
        two_sections(n) if fast else relay_shards,
        mesh=mesh,
        in_specs=(
            P(None, "dp", None, None),
            P("section", "dp", None),
            P("section", None, "dp"),
            P("section", None, "dp", None),
            P("section", None, None, "dp"),
            P("section", None),
            P(),
            P(None, "section"),
        ),
        out_specs=(P(None, "dp", "section"), P(None, "dp", "section")),
        check_vma=False,
    )
```

```python
import functools

import jax
import jax.numpy as jnp
from jax import lax
from jax.experimental import pallas as pl
from jax.experimental.pallas import tpu as pltpu
from jax.sharding import PartitionSpec as P

HEAD = 64
epsilon = 1e-06
F32, BF16 = jnp.float32, jnp.bfloat16
MESH = pl.DeviceIdType.MESH


def contract(spec, left, right):
    return jnp.einsum(spec, left, right, preferred_element_type=jnp.float32)


def norm_jvp(primal, tangents, gains):
    average = jnp.mean(primal, -1, keepdims=True)
    centred = primal - average
    inverse = lax.rsqrt(jnp.mean(centred * centred, -1, keepdims=True) + epsilon)
    dcentred = tangents - jnp.mean(tangents, -1, keepdims=True)
    dinverse = -(inverse**3) * jnp.mean(centred * dcentred, -1, keepdims=True)
    return (centred * inverse * gains, (dcentred * inverse + centred * dinverse) * gains)


def layer_step(state, qkv_weight, out_weight, value_tangent, out_tangent, gains):
    hd = out_weight.shape[0]
    heads = hd // HEAD
    resid = state.astype(F32)
    normed_zero, normed_rest = norm_jvp(resid[0], resid[1:], gains)
    normed = jnp.concatenate([normed_zero[None], normed_rest]).astype(BF16)
    streams, batch, tokens_here, width = normed.shape
    projected = contract("sbtd,de->sbte", normed, qkv_weight)
    extra_value = contract("btd,kde->kbte", normed[0], value_tangent)
    queries = projected[..., :hd]
    key_rows = projected[..., hd : 2 * hd]
    values = projected[..., 2 * hd :]
    values = jnp.concatenate([values[:1], values[1:] + extra_value])
    shape_heads = (streams, batch, tokens_here, heads, HEAD)
    queries = queries.astype(BF16).reshape(shape_heads)
    key_rows = key_rows.astype(BF16).reshape(shape_heads)
    values = values.astype(BF16).reshape(shape_heads)
    factor = HEAD ** (-0.5)
    scores = contract("bqhe,bkhe->bhqk", queries[0], key_rows[0]) * factor
    probs = jax.nn.softmax(scores, -1)
    dscores = (
        contract("sbqhe,bkhe->sbhqk", queries[1:], key_rows[0])
        + contract("bqhe,sbkhe->sbhqk", queries[0], key_rows[1:])
    ) * factor
    dprobs = probs * (dscores - jnp.sum(probs * dscores, -1, keepdims=True))
    probs_low = probs.astype(BF16)
    dprobs_low = dprobs.astype(BF16)
    attended_zero = contract("bhqk,bkhe->bqhe", probs_low, values[0])
    attended_rest = contract("sbhqk,bkhe->sbqhe", dprobs_low, values[0]) + contract(
        "bhqk,sbkhe->sbqhe", probs_low, values[1:]
    )
    attended = jnp.concatenate([attended_zero[None], attended_rest]).astype(BF16)
    attended = attended.reshape(streams, batch, tokens_here, hd)
    output = contract("sbte,ed->sbtd", attended, out_weight)
    extra_out = contract("bte,ked->kbtd", attended[0], out_tangent)
    output = jnp.concatenate([output[:1], output[1:] + extra_out])
    return (resid + output).astype(BF16)


def relay_shards(tokens, w_qkv, w_output, tangent_value, tangent_output, layer_gain, final_gain, head):
    full_qkv, full_output, full_value_tan, full_output_tan = (
        lax.all_gather(w_qkv, "dp", axis=1, tiled=True),
        lax.all_gather(w_output, "dp", axis=2, tiled=True),
        lax.all_gather(tangent_value, "dp", axis=2, tiled=True),
        lax.all_gather(tangent_output, "dp", axis=3, tiled=True),
    )
    tangents = tangent_value.shape[1]

    def advance_layer(state):
        return layer_step(
            state, full_qkv[0], full_output[0], full_value_tan[0], full_output_tan[0], layer_gain[0]
        )

    section_index = lax.axis_index("section")
    section_count = lax.axis_size("section")
    route = [(i, i + 1) for i in range(section_count - 1)]
    micro, _, toks, width = tokens.shape
    entering = jnp.concatenate(
        [tokens.reshape(1, micro, toks, width), jnp.zeros((tangents, micro, toks, width), BF16)]
    )

    def advance(step, outgoing):
        incoming = lax.ppermute(outgoing, "section", route)
        source = jnp.where(step == 0, entering, incoming)
        return lax.cond(section_index == step, advance_layer, jnp.zeros_like, source)

    finished = lax.fori_loop(0, section_count, advance, jnp.zeros_like(entering))
    collected = finished[:, :, 0, :]
    mine = section_index == section_count - 1
    features = lax.psum(jnp.where(mine, collected, jnp.zeros_like(collected)), "section")
    widened = features.astype(F32)
    final_zero, final_rest = norm_jvp(widened[0], widened[1:], final_gain)
    normed_final = jnp.concatenate([final_zero[None], final_rest]).astype(BF16)
    logits = contract("sbd,dc->sbc", normed_final, head)
    return (logits[0][:, None, :], jnp.sum(logits[1:] * logits[1:], 0)[:, None, :])


def dot(a, b):
    return lax.dot_general(a, b, (((1,), (0,)), ((), ())), preferred_element_type=F32)


def dot_t(a, b):
    return lax.dot_general(a, b, (((1,), (1,)), ((), ())), preferred_element_type=F32)


class Gather:
    def __init__(self, n, a_full, b_full, send, recv):
        self.nz = n // 4
        self.a_full, self.b_full, self.send, self.recv = a_full, b_full, send, recv
        self.rows = a_full.shape[0] // n
        self.me = lax.axis_index("dp")
        self.section = lax.axis_index("section")
        me = self.me
        self.x_near = me + 1 - 2 * (me % 2)
        self.y_near = me + 2 - 4 * ((me // 2) % 2)
        self.z = me // 4
        self.diagonal = self.x_near + self.y_near - me
        self.sends = []
        self.slot = 0

    def piece(self, src, group, half):
        depth = self.rows // 2
        at = pl.ds(pl.multiple_of(src * self.rows + half * depth, depth), depth)
        return self.a_full.at[at, :] if group == 0 else self.b_full.at[:, at, :]

    def copy(self, src, group, half, target, slot):
        ref = self.piece(src, group, half)
        return pltpu.make_async_remote_copy(
            src_ref=ref,
            dst_ref=ref,
            send_sem=self.send.at[slot],
            recv_sem=self.recv.at[src, group * 2 + half],
            device_id={"section": self.section, "dp": target},
            device_id_type=MESH,
        )

    def forward(self, cond, src, group, half, target):
        slot = self.slot
        self.slot += 1

        def go():
            self.copy(src, group, half, target, slot).start()

        def end():
            self.copy(src, group, half, target, slot).wait_send()

        if cond is None:
            go()
        else:
            pl.when(cond)(go)
        self.sends.append((cond, end))

    def arrived(self, src, group, half):
        self.copy(src, group, half, self.me, 0).wait_recv()

    def sources(self, d):
        if d == 0:
            return [(0, None)]
        return [(-d, self.z >= d), (d, self.z + d < self.nz)]

    def direct(self, group, d):
        for shift, cond in self.sources(d):
            src = self.me + 4 * shift
            for half in range(2):
                if d > 0:
                    pl.when(cond)(functools.partial(self.arrived, src, group, half))
                if shift <= 0 and d < self.nz - 1:
                    up = self.z + 1 < self.nz
                    self.forward(up if cond is None else cond & up, src, group, half, self.me + 4)
                if shift >= 0 and d < self.nz - 1:
                    down = self.z >= 1
                    self.forward(down if cond is None else cond & down, src, group, half, self.me - 4)
                order = ((self.y_near, self.x_near), (self.x_near, self.y_near))[half]
                for target in order:
                    self.forward(cond, src, group, half, target)

    def relay(self, group, d):
        for shift, cond in self.sources(d):
            for half, near, target in ((0, self.x_near, self.y_near), (1, self.y_near, self.x_near)):
                src = near + 4 * shift
                wait = functools.partial(self.arrived, src, group, half)
                wait() if cond is None else pl.when(cond)(wait)
                self.forward(cond, src, group, half, target)

    def rest(self, group):
        for z in range(self.nz):
            up = 4 * (z - self.z)
            self.arrived(self.x_near + up, group, 1)
            self.arrived(self.y_near + up, group, 0)
            self.arrived(self.diagonal + up, group, 0)
            self.arrived(self.diagonal + up, group, 1)

    def drain(self):
        for cond, end in self.sends:
            end() if cond is None else pl.when(cond)(end)
        self.sends = []


def send_slots(n):
    nz = n // 4
    return 2 * 2 * (4 + 3 * 2 * (nz - 1) + 2 * nz)


def norm_rows(x, gains):
    average = jnp.mean(x, -1, keepdims=True)
    centred = x - average
    inverse = lax.rsqrt(jnp.mean(centred * centred, -1, keepdims=True) + epsilon)
    return centred, inverse, centred * inverse * gains


def norm_tangent(t, centred, inverse, gains):
    dcentred = t - jnp.mean(t, -1, keepdims=True)
    dinverse = -(inverse * inverse * inverse) * jnp.mean(centred * dcentred, -1, keepdims=True)
    return (dcentred * inverse + centred * dinverse) * gains


def softmax(scores):
    e = jnp.exp(scores - jnp.max(scores, -1, keepdims=True))
    return e / jnp.sum(e, -1, keepdims=True)


def first_norm(sizes, tokens, gain, normed):
    micro, toks, width, hd, tangents = sizes
    for b in range(micro):
        x = tokens[b].astype(F32)
        normed[0, pl.ds(b * toks, toks), :] = norm_rows(x, gain[...])[2].astype(BF16)


def first_qkv(sizes, a_full, normed, proj):
    micro, toks, width, hd, tangents = sizes
    n = normed[0]
    for c in range(3 + tangents):
        at = pl.ds(c * hd, hd)
        proj[:, at] = dot(n, a_full[:, at]).astype(BF16)


def first_attend(sizes, proj, att, b):
    micro, toks, width, hd, tangents = sizes
    factor = HEAD ** (-0.5)
    even = lax.broadcasted_iota(jnp.int32, (toks, 2 * HEAD), 1) < HEAD
    rows = pl.ds(b * toks, toks)
    for pair in range(hd // (2 * HEAD)):
        lanes = pair * 2 * HEAD
        q = proj[rows, pl.ds(lanes, 2 * HEAD)]
        k = proj[rows, pl.ds(hd + lanes, 2 * HEAD)]
        vs = [proj[rows, pl.ds((2 + s) * hd + lanes, 2 * HEAD)] for s in range(1 + tangents)]
        zero = jnp.zeros_like(q)
        low = []
        for mine in (jnp.where(even, q, zero), jnp.where(even, zero, q)):
            low.append(softmax(dot_t(mine, k) * factor).astype(BF16))
        for s, v in enumerate(vs):
            joined = jnp.where(even, dot(low[0], v), dot(low[1], v))
            at = pl.ds((s * micro + b) * toks, toks)
            att[at, pl.ds(lanes, 2 * HEAD)] = joined.astype(BF16)


def first_out(sizes, tokens, b_full, att, state):
    micro, toks, width, hd, tangents = sizes
    rows0 = micro * toks
    tile = 256
    for c in range(width // tile):
        at = pl.ds(c * tile, tile)
        out = dot_t(att[...], b_full[0, at, :])
        extra = [dot_t(att[pl.ds(0, rows0), :], b_full[1 + j, at, :]) for j in range(tangents)]
        for b in range(micro):
            x = tokens[b, :, at].astype(F32)
            state[pl.ds(b * toks, toks), at] = (x + out[b * toks : (b + 1) * toks]).astype(BF16)
        for j in range(tangents):
            state[pl.ds((1 + j) * rows0, rows0), at] = (
                out[(1 + j) * rows0 : (2 + j) * rows0] + extra[j]
            ).astype(BF16)


BLOCK = 16


class Plane:
    def __init__(self, g, send, recv):
        self.g, self.send, self.recv = g, send, recv
        self.place = g.me % 4
        self.peers = (g.diagonal, g.x_near, g.y_near)

    def copy(self, stage, i, src, dst, source):
        return pltpu.make_async_remote_copy(
            src_ref=src,
            dst_ref=dst,
            send_sem=self.send.at[stage, i],
            recv_sem=self.recv.at[stage, source],
            device_id={"section": self.g.section, "dp": self.peers[i]},
            device_id_type=MESH,
        )

    def exchange(self, stage, out_of, into):
        for i, peer in enumerate(self.peers):
            self.copy(stage, i, out_of(peer % 4), into(self.place), self.place).start()

    def arrive(self, stage, out_of, into):
        for i, peer in enumerate(self.peers):
            self.copy(stage, i, out_of(peer % 4), into(peer % 4), peer % 4).wait_recv()

    def finish(self, stage, out_of, into):
        for i, peer in enumerate(self.peers):
            self.copy(stage, i, out_of(peer % 4), into(self.place), self.place).wait_send()


class Line:
    def __init__(self, g, parts, send, recv):
        self.g, self.parts, self.send, self.recv = g, parts, send, recv
        self.sends = []

    def copy(self, z, group, way, target):
        rows = 4 * self.g.rows
        at = pl.ds(pl.multiple_of(z * rows, rows), rows)
        ref = self.parts[0].at[at, :] if group == 0 else self.parts[1].at[:, at, :]
        return pltpu.make_async_remote_copy(
            src_ref=ref,
            dst_ref=ref,
            send_sem=self.send.at[z, 2 * group + way],
            recv_sem=self.recv.at[z, group],
            device_id={"section": self.g.section, "dp": target},
            device_id_type=MESH,
        )

    def run(self, group):
        g = self.g
        for d in range(g.nz):
            for shift, cond in g.sources(d):
                z = g.z + shift

                def step(z=z, shift=shift, d=d):
                    if d > 0:
                        self.copy(z, group, 0, g.me).wait_recv()
                    if shift <= 0 and d < g.nz - 1:
                        pl.when(g.z + 1 < g.nz)(lambda: self.copy(z, group, 0, g.me + 4).start())
                    if shift >= 0 and d < g.nz - 1:
                        pl.when(g.z >= 1)(lambda: self.copy(z, group, 1, g.me - 4).start())

                step() if cond is None else pl.when(cond)(step)

    def drain(self, group):
        g = self.g
        for d in range(g.nz - 1):
            for shift, cond in g.sources(d):
                z = g.z + shift

                def step(z=z, shift=shift):
                    if shift <= 0:
                        pl.when(g.z + 1 < g.nz)(lambda: self.copy(z, group, 0, g.me + 4).wait_send())
                    if shift >= 0:
                        pl.when(g.z >= 1)(lambda: self.copy(z, group, 1, g.me - 4).wait_send())

                step() if cond is None else pl.when(cond)(step)


def class_rows(sizes, gain, state):
    micro, toks, width, hd, tangents = sizes
    streams = 1 + tangents
    rows0 = micro * toks
    filler = [jnp.zeros((BLOCK - micro * streams, width), F32)]
    heads_of = [
        state[pl.ds(s * rows0 + b * toks, 16), :].astype(F32)[:1] for s in range(streams) for b in range(micro)
    ]
    resid = jnp.concatenate(heads_of + filler, 0)
    primal = jnp.concatenate(heads_of[:micro] * streams + filler, 0)
    centred, inverse, y = norm_rows(primal, gain[...])
    dy = norm_tangent(resid, centred, inverse, gain[...])
    which = lax.broadcasted_iota(jnp.int32, resid.shape, 0)
    return resid, jnp.where(which < micro, y, dy).astype(BF16)


def last_norm(sizes, gain, state, normed):
    micro, toks, width, hd, tangents = sizes
    rows0 = micro * toks
    for b in range(micro):
        at = pl.ds(b * toks, toks)
        centred, inverse, y = norm_rows(state[at, :].astype(F32), gain[...])
        normed[0, at, :] = y.astype(BF16)
        for j in range(tangents):
            t = state[pl.ds((1 + j) * rows0 + b * toks, toks), :].astype(F32)
            normed[1 + j, at, :] = norm_tangent(t, centred, inverse, gain[...]).astype(BF16)


def last_attend(sizes, heads, u, normed):
    micro, toks, width, hd, tangents = sizes
    streams = 1 + tangents
    factor = HEAD ** (-0.5)
    sums = []
    for b in range(micro):
        at = pl.ds(b * toks, toks)
        ub = u[b * streams * heads : (b + 1) * streams * heads].astype(BF16)
        base = dot_t(ub, normed[0, at, :]) * factor
        u0 = ub[:heads]
        probs = softmax(base[:heads])
        weights = [probs]
        for j in range(tangents):
            ds = base[(1 + j) * heads : (2 + j) * heads] + dot_t(u0, normed[1 + j, at, :]) * factor
            weights.append(probs * (ds - jnp.sum(probs * ds, -1, keepdims=True)))
        m = dot(jnp.concatenate(weights, 0).astype(BF16), normed[0, at, :])
        low = probs.astype(BF16)
        parts = [m[:heads]]
        for j in range(tangents):
            parts.append(m[(1 + j) * heads : (2 + j) * heads] + dot(low, normed[1 + j, at, :]))
        sums += parts
    return jnp.concatenate(sums, 0).astype(BF16)


def order(sizes, heads, flip):
    micro, toks, width, hd, tangents = sizes
    streams = 1 + tangents
    share = heads // 4
    few, many = micro * streams * heads, heads * BLOCK
    shape = (many, few) if flip else (few, many)
    r = lax.broadcasted_iota(jnp.int32, shape, 1 if flip else 0)
    c = lax.broadcasted_iota(jnp.int32, shape, 0 if flip else 1)
    head, i = r % heads, r // heads
    i = (i % streams) * micro + i // streams
    return (c == head * BLOCK + i).astype(F32).astype(BF16)


def lowered(extra, micro, rows):
    width = extra[0].shape[-1]
    parts = [jnp.zeros((micro, width), F32)] + [e[:micro] for e in extra]
    used = micro * len(parts)
    return jnp.concatenate(parts + [jnp.zeros((rows - used, width), F32)], 0)


def kernel(
    n, sizes, tokens, w_qkv, tangent_value, outs, gain, final_gain, head, mean_ref, var_ref,
    a_full, b_full, normed, proj, att, state, state_in, classes, classes_in,
    a_quarter, b_quarter, a_part, b_part, cls_all, u_out, u_all, m_out, m_all, o_out, o_all,
    send, recv, local, gate, core_sems, plane_send, plane_recv, line_send, line_recv,
):
    micro, toks, width, hd, tangents = sizes
    streams = 1 + tangents
    heads = hd // HEAD
    share = heads // 4
    part = share * HEAD
    g = Gather(n, a_full, b_full, send, recv)
    me, section = g.me, g.section
    other = 1 - section
    up, down = g.z + 1 < g.nz, g.z >= 1
    plane = Plane(g, plane_send, plane_recv)
    line = Line(g, (a_part, b_part), line_send, line_recv)

    barrier = pltpu.get_barrier_semaphore()

    def greet(target, sec):
        pl.semaphore_signal(
            barrier, inc=1, device_id={"section": sec, "dp": target}, device_id_type=MESH
        )

    for near in (g.x_near, g.y_near, g.diagonal):
        greet(near, section)
    greet(me, other)
    pl.when(up)(lambda: greet(me + 4, section))
    pl.when(down)(lambda: greet(me - 4, section))

    def met():
        if g.nz > 1:
            middle = up & down
            pl.when(middle)(lambda: pl.semaphore_wait(barrier, 6))
            pl.when(jnp.logical_not(middle))(lambda: pl.semaphore_wait(barrier, 5))
        else:
            pl.semaphore_wait(barrier, 4)

    def across(src, dst, i):
        return pltpu.make_async_remote_copy(
            src_ref=src,
            dst_ref=dst,
            send_sem=core_sems.at[2 * i],
            recv_sem=core_sems.at[2 * i + 1],
            device_id={"section": other, "dp": me},
            device_id_type=MESH,
        )

    own = pl.ds(pl.multiple_of(me * g.rows, g.rows), g.rows)

    def moved(pairs):
        moves = [pltpu.make_async_copy(src, dst, local.at[i]) for i, (src, dst) in enumerate(pairs)]
        for move in moves:
            move.start()
        for move in moves:
            move.wait()

    met()

    @pl.when(section == 0)
    def _():
        pairs = [(w_qkv, a_full.at[own, pl.ds(0, 3 * hd)])]
        for j in range(tangents):
            pairs.append((tangent_value.at[j], a_full.at[own, pl.ds((3 + j) * hd, hd)]))
        pairs.append((outs, b_full.at[:, own, :]))
        moved(pairs)
        steps = [(group, d) for group in range(2) for d in range(g.nz)]
        g.direct(*steps[0])
        first_norm(sizes, tokens, gain, normed)
        for i, step in enumerate(steps):
            if step == (1, 0):
                g.rest(0)
                first_qkv(sizes, a_full, normed, proj)
            if step[0] == 1 and 1 <= step[1] <= micro:
                first_attend(sizes, proj, att, step[1] - 1)
            if i + 1 < len(steps):
                g.direct(*steps[i + 1])
            if i + 1 == g.nz + min(1, g.nz - 1):
                pl.semaphore_signal(
                    gate, inc=1, device_id={"section": other, "dp": me}, device_id_type=MESH
                )
            g.relay(*step)
        for b in range(g.nz - 1, micro):
            first_attend(sizes, proj, att, b)
        g.rest(1)
        first_out(sizes, tokens, b_full, att, state)
        onward = across(state, state_in, 0)
        onward.start()
        g.drain()
        onward.wait_send()
        across(classes, classes_in, 1).wait_recv()

    @pl.when(section == 1)
    def _():
        pairs = []
        for p in range(4):
            for m in range(3):
                pairs.append(
                    (w_qkv.at[:, pl.ds(m * hd + p * part, part)], a_quarter.at[p, :, pl.ds(m * part, part)])
                )
            for j in range(tangents):
                pairs.append(
                    (
                        tangent_value.at[j, :, pl.ds(p * part, part)],
                        a_quarter.at[p, :, pl.ds((3 + j) * part, part)],
                    )
                )
            pairs.append((outs.at[:, :, pl.ds(p * part, part)], b_quarter.at[p]))
        moved(pairs)

        def at_place(place):
            row = (g.z * 4 + place) * g.rows
            return pl.ds(pl.multiple_of(row, g.rows), g.rows)

        stages = [
            (0, lambda p: a_quarter.at[p], lambda p: a_part.at[at_place(p), :]),
            (1, lambda p: b_quarter.at[p], lambda p: b_part.at[:, at_place(p), :]),
            (2, lambda p: cls_all.at[plane.place], lambda p: cls_all.at[p]),
            (3, lambda p: u_out.at[p], lambda p: u_all.at[p]),
            (4, lambda p: m_out.at[p], lambda p: m_all.at[p]),
            (5, lambda p: o_out.at[p], lambda p: o_all.at[p]),
        ]
        for stage in stages[:2]:
            plane.exchange(*stage)
        moved(
            [
                (a_quarter.at[plane.place], a_part.at[own, :]),
                (b_quarter.at[plane.place], b_part.at[:, own, :]),
            ]
        )
        for stage in stages[:2]:
            plane.arrive(*stage)
        pl.semaphore_wait(gate, 1)
        line.run(0)
        line.run(1)

        across(state, state_in, 0).wait_recv()
        resid, firsts = class_rows(sizes, gain, state_in)
        cls_all[plane.place] = firsts
        plane.exchange(*stages[2])
        last_norm(sizes, gain, state_in, normed)
        plane.arrive(*stages[2])
        rows = jnp.concatenate([cls_all[k] for k in range(4)], 0)
        q = dot(rows, a_part[:, pl.ds(0, part)]).astype(BF16)
        owner = lax.broadcasted_iota(jnp.int32, (BLOCK, part), 1) // HEAD
        zero = jnp.zeros((BLOCK, part), F32)
        spread = []
        for k in range(4):
            block = q[k * BLOCK : (k + 1) * BLOCK].astype(F32)
            spread += [jnp.where(owner == h, block, zero) for h in range(share)]
        u = dot_t(jnp.concatenate(spread, 0).astype(BF16), a_part[:, pl.ds(part, part)]).astype(BF16)
        tall = share * BLOCK
        for k in range(4):
            u_out[k] = u[k * tall : (k + 1) * tall]
        plane.exchange(*stages[3])
        u_all[plane.place] = u_out[plane.place]
        plane.arrive(*stages[3])
        u48 = dot(order(sizes, heads, False), jnp.concatenate([u_all[k] for k in range(4)], 0))
        sums = last_attend(sizes, heads, u48, normed)
        spreadm = dot(order(sizes, heads, True), sums).astype(BF16)
        for k in range(4):
            m_out[k] = spreadm[k * tall : (k + 1) * tall]
        plane.exchange(*stages[4])
        m_all[plane.place] = m_out[plane.place]
        plane.arrive(*stages[4])
        m = jnp.concatenate([m_all[k] for k in range(4)], 0)
        r = [dot(m, a_part[:, pl.ds((2 + c) * part, part)]) for c in range(streams)]

        def picked(x, k):
            chosen = zero
            for h in range(share):
                at = k * tall + h * BLOCK
                chosen = jnp.where(owner == h, x[at : at + BLOCK], chosen)
            return chosen

        attended = jnp.concatenate(
            [
                picked(r[0], k) + lowered([picked(x, k) for x in r[1:]], micro, BLOCK)
                for k in range(4)
            ],
            0,
        ).astype(BF16)
        out = [dot_t(attended, b_part[c]) for c in range(streams)]
        some = o_out.shape[1]
        for k in range(4):
            at = k * BLOCK
            extra = [x[at : at + micro] for x in out[1:]]
            o_out[k] = out[0][at : at + some] + lowered(extra, micro, some)
        plane.exchange(*stages[5])
        o_all[plane.place] = o_out[plane.place]
        plane.arrive(*stages[5])
        total = o_all[0] + o_all[1] + o_all[2] + o_all[3]
        final = (resid[:some] + total).astype(BF16).astype(F32)
        classes[...] = final
        back = across(classes, classes_in, 1)
        back.start()
        classes_in[...] = final
        for stage in stages:
            plane.finish(*stage)
        line.drain(0)
        line.drain(1)
        back.wait_send()

    rows = classes_in[...]
    count = classes_in.shape[0]
    primal = jnp.concatenate([rows[:micro]] * (1 + tangents) + [rows[(1 + tangents) * micro :]], 0)
    centred, inverse, y = norm_rows(primal, final_gain[...])
    dy = norm_tangent(rows, centred, inverse, final_gain[...])
    which = lax.broadcasted_iota(jnp.int32, (count, width), 0)
    logits = dot_t(jnp.where(which < micro, y, dy).astype(BF16), head[...])
    mean_ref[...] = logits[:micro]
    var_ref[...] = sum(
        logits[(1 + j) * micro : (2 + j) * micro] * logits[(1 + j) * micro : (2 + j) * micro]
        for j in range(tangents)
    )


def two_sections(n):
    def shards(tokens, w_qkv, w_output, tangent_value, tangent_output, layer_gain, final_gain, head):
        micro, _, toks, width = tokens.shape
        tangents = tangent_value.shape[1]
        hd = w_output.shape[1]
        classes = head.shape[1]
        rows = width // n
        outs = jnp.swapaxes(jnp.concatenate([w_output, tangent_output[0]], 0), 1, 2)
        sizes = (micro, toks, width, hd, tangents)
        vmem = pl.BlockSpec(memory_space=pltpu.VMEM)
        anywhere = pl.BlockSpec(memory_space=pl.ANY)
        streams = 1 + tangents
        padded = -(-micro * streams // 8) * 8
        all_rows = streams * micro * toks
        tall = hd // HEAD // 4 * BLOCK
        mean, var = pl.pallas_call(
            functools.partial(kernel, n, sizes),
            out_shape=[jax.ShapeDtypeStruct((micro, classes), F32)] * 2,
            in_specs=[vmem, anywhere, anywhere, anywhere, vmem, vmem, vmem],
            out_specs=[vmem, vmem],
            scratch_shapes=[
                pltpu.VMEM((width, (3 + tangents) * hd), BF16),
                pltpu.VMEM((streams, width, hd), BF16),
                pltpu.VMEM((streams, micro * toks, width), BF16),
                pltpu.VMEM((micro * toks, (3 + tangents) * hd), BF16),
                pltpu.VMEM((all_rows, hd), BF16),
                pltpu.VMEM((all_rows, width), BF16),
                pltpu.VMEM((all_rows, width), BF16),
                pltpu.VMEM((padded, width), F32),
                pltpu.VMEM((padded, width), F32),
                pltpu.VMEM((4, rows, (3 + tangents) * hd // 4), BF16),
                pltpu.VMEM((4, streams, rows, hd // 4), BF16),
                pltpu.VMEM((width, (3 + tangents) * hd // 4), BF16),
                pltpu.VMEM((streams, width, hd // 4), BF16),
                pltpu.VMEM((4, BLOCK, width), BF16),
                pltpu.VMEM((4, tall, width), BF16),
                pltpu.VMEM((4, tall, width), BF16),
                pltpu.VMEM((4, tall, width), BF16),
                pltpu.VMEM((4, tall, width), BF16),
                pltpu.VMEM((4, padded, width), F32),
                pltpu.VMEM((4, padded, width), F32),
                pltpu.SemaphoreType.DMA((send_slots(n),)),
                pltpu.SemaphoreType.DMA((n, 4)),
                pltpu.SemaphoreType.DMA((4 * (4 + tangents),)),
                pltpu.SemaphoreType.REGULAR,
                pltpu.SemaphoreType.DMA((4,)),
                pltpu.SemaphoreType.DMA((6, 3)),
                pltpu.SemaphoreType.DMA((6, 4)),
                pltpu.SemaphoreType.DMA((n // 4, 4)),
                pltpu.SemaphoreType.DMA((n // 4, 2)),
            ],
            compiler_params=pltpu.CompilerParams(
                collective_id=0, has_side_effects=True, vmem_limit_bytes=60 * 2**20
            ),
        )(
            tokens.reshape(micro, toks, width),
            w_qkv[0],
            tangent_value[0],
            outs,
            layer_gain,
            final_gain[None],
            head.T,
        )
        return mean[:, None, :], var[:, None, :]

    return shards


def solution(mesh):
    n = mesh.shape["dp"]
    fast = mesh.shape["section"] == 2 and n % 4 == 0
    return jax.shard_map(
        two_sections(n) if fast else relay_shards,
        mesh=mesh,
        in_specs=(
            P(None, "dp", None, None),
            P("section", "dp", None),
            P("section", None, "dp"),
            P("section", None, "dp", None),
            P("section", None, None, "dp"),
            P("section", None),
            P(),
            P(None, "section"),
        ),
        out_specs=(P(None, "dp", "section"), P(None, "dp", "section")),
        check_vma=False,
    )
```

```python
import functools

import jax
import jax.numpy as jnp
from jax import lax
from jax.experimental import pallas as pl
from jax.experimental.pallas import tpu as pltpu
from jax.sharding import PartitionSpec as P

HEAD = 64
epsilon = 1e-06
F32, BF16 = jnp.float32, jnp.bfloat16
MESH = pl.DeviceIdType.MESH


def contract(spec, left, right):
    return jnp.einsum(spec, left, right, preferred_element_type=jnp.float32)


def norm_jvp(primal, tangents, gains):
    average = jnp.mean(primal, -1, keepdims=True)
    centred = primal - average
    inverse = lax.rsqrt(jnp.mean(centred * centred, -1, keepdims=True) + epsilon)
    dcentred = tangents - jnp.mean(tangents, -1, keepdims=True)
    dinverse = -(inverse**3) * jnp.mean(centred * dcentred, -1, keepdims=True)
    return (centred * inverse * gains, (dcentred * inverse + centred * dinverse) * gains)


def layer_step(state, qkv_weight, out_weight, value_tangent, out_tangent, gains):
    hd = out_weight.shape[0]
    heads = hd // HEAD
    resid = state.astype(F32)
    normed_zero, normed_rest = norm_jvp(resid[0], resid[1:], gains)
    normed = jnp.concatenate([normed_zero[None], normed_rest]).astype(BF16)
    streams, batch, tokens_here, width = normed.shape
    projected = contract("sbtd,de->sbte", normed, qkv_weight)
    extra_value = contract("btd,kde->kbte", normed[0], value_tangent)
    queries = projected[..., :hd]
    key_rows = projected[..., hd : 2 * hd]
    values = projected[..., 2 * hd :]
    values = jnp.concatenate([values[:1], values[1:] + extra_value])
    shape_heads = (streams, batch, tokens_here, heads, HEAD)
    queries = queries.astype(BF16).reshape(shape_heads)
    key_rows = key_rows.astype(BF16).reshape(shape_heads)
    values = values.astype(BF16).reshape(shape_heads)
    factor = HEAD ** (-0.5)
    scores = contract("bqhe,bkhe->bhqk", queries[0], key_rows[0]) * factor
    probs = jax.nn.softmax(scores, -1)
    dscores = (
        contract("sbqhe,bkhe->sbhqk", queries[1:], key_rows[0])
        + contract("bqhe,sbkhe->sbhqk", queries[0], key_rows[1:])
    ) * factor
    dprobs = probs * (dscores - jnp.sum(probs * dscores, -1, keepdims=True))
    probs_low = probs.astype(BF16)
    dprobs_low = dprobs.astype(BF16)
    attended_zero = contract("bhqk,bkhe->bqhe", probs_low, values[0])
    attended_rest = contract("sbhqk,bkhe->sbqhe", dprobs_low, values[0]) + contract(
        "bhqk,sbkhe->sbqhe", probs_low, values[1:]
    )
    attended = jnp.concatenate([attended_zero[None], attended_rest]).astype(BF16)
    attended = attended.reshape(streams, batch, tokens_here, hd)
    output = contract("sbte,ed->sbtd", attended, out_weight)
    extra_out = contract("bte,ked->kbtd", attended[0], out_tangent)
    output = jnp.concatenate([output[:1], output[1:] + extra_out])
    return (resid + output).astype(BF16)


def relay_shards(tokens, w_qkv, w_output, tangent_value, tangent_output, layer_gain, final_gain, head):
    full_qkv, full_output, full_value_tan, full_output_tan = (
        lax.all_gather(w_qkv, "dp", axis=1, tiled=True),
        lax.all_gather(w_output, "dp", axis=2, tiled=True),
        lax.all_gather(tangent_value, "dp", axis=2, tiled=True),
        lax.all_gather(tangent_output, "dp", axis=3, tiled=True),
    )
    tangents = tangent_value.shape[1]

    def advance_layer(state):
        return layer_step(
            state, full_qkv[0], full_output[0], full_value_tan[0], full_output_tan[0], layer_gain[0]
        )

    section_index = lax.axis_index("section")
    section_count = lax.axis_size("section")
    route = [(i, i + 1) for i in range(section_count - 1)]
    micro, _, toks, width = tokens.shape
    entering = jnp.concatenate(
        [tokens.reshape(1, micro, toks, width), jnp.zeros((tangents, micro, toks, width), BF16)]
    )

    def advance(step, outgoing):
        incoming = lax.ppermute(outgoing, "section", route)
        source = jnp.where(step == 0, entering, incoming)
        return lax.cond(section_index == step, advance_layer, jnp.zeros_like, source)

    finished = lax.fori_loop(0, section_count, advance, jnp.zeros_like(entering))
    collected = finished[:, :, 0, :]
    mine = section_index == section_count - 1
    features = lax.psum(jnp.where(mine, collected, jnp.zeros_like(collected)), "section")
    widened = features.astype(F32)
    final_zero, final_rest = norm_jvp(widened[0], widened[1:], final_gain)
    normed_final = jnp.concatenate([final_zero[None], final_rest]).astype(BF16)
    logits = contract("sbd,dc->sbc", normed_final, head)
    return (logits[0][:, None, :], jnp.sum(logits[1:] * logits[1:], 0)[:, None, :])


def dot(a, b):
    return lax.dot_general(a, b, (((1,), (0,)), ((), ())), preferred_element_type=F32)


def dot_t(a, b):
    return lax.dot_general(a, b, (((1,), (1,)), ((), ())), preferred_element_type=F32)


class Gather:
    def __init__(self, n, a_full, b_full, send, recv):
        self.nz = n // 4
        self.a_full, self.b_full, self.send, self.recv = a_full, b_full, send, recv
        self.rows = a_full.shape[0] // n
        self.me = lax.axis_index("dp")
        self.section = lax.axis_index("section")
        me = self.me
        self.x_near = me + 1 - 2 * (me % 2)
        self.y_near = me + 2 - 4 * ((me // 2) % 2)
        self.z = me // 4
        self.diagonal = self.x_near + self.y_near - me
        self.sends = []
        self.slot = 0

    def piece(self, src, group, half):
        depth = self.rows // 2
        at = pl.ds(pl.multiple_of(src * self.rows + half * depth, depth), depth)
        return self.a_full.at[at, :] if group == 0 else self.b_full.at[:, at, :]

    def copy(self, src, group, half, target, slot):
        ref = self.piece(src, group, half)
        return pltpu.make_async_remote_copy(
            src_ref=ref,
            dst_ref=ref,
            send_sem=self.send.at[slot],
            recv_sem=self.recv.at[src, group * 2 + half],
            device_id={"section": self.section, "dp": target},
            device_id_type=MESH,
        )

    def forward(self, cond, src, group, half, target):
        slot = self.slot
        self.slot += 1

        def go():
            self.copy(src, group, half, target, slot).start()

        def end():
            self.copy(src, group, half, target, slot).wait_send()

        if cond is None:
            go()
        else:
            pl.when(cond)(go)
        self.sends.append((cond, end))

    def arrived(self, src, group, half):
        self.copy(src, group, half, self.me, 0).wait_recv()

    def sources(self, d):
        if d == 0:
            return [(0, None)]
        return [(-d, self.z >= d), (d, self.z + d < self.nz)]

    def direct(self, group, d):
        for shift, cond in self.sources(d):
            src = self.me + 4 * shift
            for half in range(2):
                if d > 0:
                    pl.when(cond)(functools.partial(self.arrived, src, group, half))
                if shift <= 0 and d < self.nz - 1:
                    up = self.z + 1 < self.nz
                    self.forward(up if cond is None else cond & up, src, group, half, self.me + 4)
                if shift >= 0 and d < self.nz - 1:
                    down = self.z >= 1
                    self.forward(down if cond is None else cond & down, src, group, half, self.me - 4)
                order = ((self.y_near, self.x_near), (self.x_near, self.y_near))[half]
                for target in order:
                    self.forward(cond, src, group, half, target)

    def relay(self, group, d):
        for shift, cond in self.sources(d):
            for half, near, target in ((0, self.x_near, self.y_near), (1, self.y_near, self.x_near)):
                src = near + 4 * shift
                wait = functools.partial(self.arrived, src, group, half)
                wait() if cond is None else pl.when(cond)(wait)
                self.forward(cond, src, group, half, target)

    def rest(self, group):
        for z in range(self.nz):
            up = 4 * (z - self.z)
            self.arrived(self.x_near + up, group, 1)
            self.arrived(self.y_near + up, group, 0)
            self.arrived(self.diagonal + up, group, 0)
            self.arrived(self.diagonal + up, group, 1)

    def drain(self):
        for cond, end in self.sends:
            end() if cond is None else pl.when(cond)(end)
        self.sends = []


def send_slots(n):
    nz = n // 4
    return 2 * 2 * (4 + 3 * 2 * (nz - 1) + 2 * nz)


def norm_rows(x, gains):
    average = jnp.mean(x, -1, keepdims=True)
    centred = x - average
    inverse = lax.rsqrt(jnp.mean(centred * centred, -1, keepdims=True) + epsilon)
    return centred, inverse, centred * inverse * gains


def norm_tangent(t, centred, inverse, gains):
    dcentred = t - jnp.mean(t, -1, keepdims=True)
    dinverse = -(inverse * inverse * inverse) * jnp.mean(centred * dcentred, -1, keepdims=True)
    return (dcentred * inverse + centred * dinverse) * gains


def softmax(scores):
    e = jnp.exp(scores - jnp.max(scores, -1, keepdims=True))
    return e / jnp.sum(e, -1, keepdims=True)


def first_norm(sizes, tokens, gain, normed):
    micro, toks, width, hd, tangents = sizes
    for b in range(micro):
        x = tokens[b].astype(F32)
        normed[0, pl.ds(b * toks, toks), :] = norm_rows(x, gain[...])[2].astype(BF16)


def first_qkv(sizes, a_full, normed, proj):
    micro, toks, width, hd, tangents = sizes
    n = normed[0]
    for c in range(3 + tangents):
        at = pl.ds(c * hd, hd)
        proj[:, at] = dot(n, a_full[:, at]).astype(BF16)


def first_attend(sizes, proj, att, b):
    micro, toks, width, hd, tangents = sizes
    factor = HEAD ** (-0.5)
    even = lax.broadcasted_iota(jnp.int32, (toks, 2 * HEAD), 1) < HEAD
    rows = pl.ds(b * toks, toks)
    for pair in range(hd // (2 * HEAD)):
        lanes = pair * 2 * HEAD
        q = proj[rows, pl.ds(lanes, 2 * HEAD)]
        k = proj[rows, pl.ds(hd + lanes, 2 * HEAD)]
        vs = [proj[rows, pl.ds((2 + s) * hd + lanes, 2 * HEAD)] for s in range(1 + tangents)]
        zero = jnp.zeros_like(q)
        low = []
        for mine in (jnp.where(even, q, zero), jnp.where(even, zero, q)):
            low.append(softmax(dot_t(mine, k) * factor).astype(BF16))
        for s, v in enumerate(vs):
            joined = jnp.where(even, dot(low[0], v), dot(low[1], v))
            at = pl.ds((s * micro + b) * toks, toks)
            att[at, pl.ds(lanes, 2 * HEAD)] = joined.astype(BF16)


def first_out(sizes, tokens, b_full, att, state):
    micro, toks, width, hd, tangents = sizes
    rows0 = micro * toks
    tile = 256
    for c in range(width // tile):
        at = pl.ds(c * tile, tile)
        out = dot_t(att[...], b_full[0, at, :])
        extra = [dot_t(att[pl.ds(0, rows0), :], b_full[1 + j, at, :]) for j in range(tangents)]
        for b in range(micro):
            x = tokens[b, :, at].astype(F32)
            state[pl.ds(b * toks, toks), at] = (x + out[b * toks : (b + 1) * toks]).astype(BF16)
        for j in range(tangents):
            state[pl.ds((1 + j) * rows0, rows0), at] = (
                out[(1 + j) * rows0 : (2 + j) * rows0] + extra[j]
            ).astype(BF16)


BLOCK = 16


class Plane:
    def __init__(self, g, send, recv):
        self.g, self.send, self.recv = g, send, recv
        self.place = g.me % 4
        self.peers = (g.diagonal, g.x_near, g.y_near)

    def copy(self, stage, i, src, dst, source):
        return pltpu.make_async_remote_copy(
            src_ref=src,
            dst_ref=dst,
            send_sem=self.send.at[stage, i],
            recv_sem=self.recv.at[stage, source],
            device_id={"section": self.g.section, "dp": self.peers[i]},
            device_id_type=MESH,
        )

    def exchange(self, stage, out_of, into):
        for i, peer in enumerate(self.peers):
            self.copy(stage, i, out_of(peer % 4), into(self.place), self.place).start()

    def arrive(self, stage, out_of, into):
        for i, peer in enumerate(self.peers):
            self.copy(stage, i, out_of(peer % 4), into(peer % 4), peer % 4).wait_recv()

    def finish(self, stage, out_of, into):
        for i, peer in enumerate(self.peers):
            self.copy(stage, i, out_of(peer % 4), into(self.place), self.place).wait_send()


class Line:
    def __init__(self, g, parts, send, recv):
        self.g, self.parts, self.send, self.recv = g, parts, send, recv
        self.sends = []

    def copy(self, z, group, way, target):
        rows = 4 * self.g.rows
        at = pl.ds(pl.multiple_of(z * rows, rows), rows)
        ref = self.parts[0].at[at, :] if group == 0 else self.parts[1].at[:, at, :]
        return pltpu.make_async_remote_copy(
            src_ref=ref,
            dst_ref=ref,
            send_sem=self.send.at[z, 2 * group + way],
            recv_sem=self.recv.at[z, group],
            device_id={"section": self.g.section, "dp": target},
            device_id_type=MESH,
        )

    def run(self, group):
        g = self.g
        for d in range(g.nz):
            for shift, cond in g.sources(d):
                z = g.z + shift

                def step(z=z, shift=shift, d=d):
                    if d > 0:
                        self.copy(z, group, 0, g.me).wait_recv()
                    if shift <= 0 and d < g.nz - 1:
                        pl.when(g.z + 1 < g.nz)(lambda: self.copy(z, group, 0, g.me + 4).start())
                    if shift >= 0 and d < g.nz - 1:
                        pl.when(g.z >= 1)(lambda: self.copy(z, group, 1, g.me - 4).start())

                step() if cond is None else pl.when(cond)(step)

    def drain(self, group):
        g = self.g
        for d in range(g.nz - 1):
            for shift, cond in g.sources(d):
                z = g.z + shift

                def step(z=z, shift=shift):
                    if shift <= 0:
                        pl.when(g.z + 1 < g.nz)(lambda: self.copy(z, group, 0, g.me + 4).wait_send())
                    if shift >= 0:
                        pl.when(g.z >= 1)(lambda: self.copy(z, group, 1, g.me - 4).wait_send())

                step() if cond is None else pl.when(cond)(step)


def class_rows(sizes, gain, state):
    micro, toks, width, hd, tangents = sizes
    streams = 1 + tangents
    rows0 = micro * toks
    filler = [jnp.zeros((BLOCK - micro * streams, width), F32)]
    heads_of = [
        state[pl.ds(s * rows0 + b * toks, 16), :].astype(F32)[:1] for s in range(streams) for b in range(micro)
    ]
    resid = jnp.concatenate(heads_of + filler, 0)
    primal = jnp.concatenate(heads_of[:micro] * streams + filler, 0)
    centred, inverse, y = norm_rows(primal, gain[...])
    dy = norm_tangent(resid, centred, inverse, gain[...])
    which = lax.broadcasted_iota(jnp.int32, resid.shape, 0)
    return resid, jnp.where(which < micro, y, dy).astype(BF16)


def last_norm(sizes, gain, state, normed):
    micro, toks, width, hd, tangents = sizes
    rows0 = micro * toks
    for b in range(micro):
        at = pl.ds(b * toks, toks)
        centred, inverse, y = norm_rows(state[at, :].astype(F32), gain[...])
        normed[0, at, :] = y.astype(BF16)
        for j in range(tangents):
            t = state[pl.ds((1 + j) * rows0 + b * toks, toks), :].astype(F32)
            normed[1 + j, at, :] = norm_tangent(t, centred, inverse, gain[...]).astype(BF16)


def last_attend(sizes, heads, u, normed):
    micro, toks, width, hd, tangents = sizes
    streams = 1 + tangents
    factor = HEAD ** (-0.5)
    sums = []
    for b in range(micro):
        at = pl.ds(b * toks, toks)
        ub = u[b * streams * heads : (b + 1) * streams * heads].astype(BF16)
        base = dot_t(ub, normed[0, at, :]) * factor
        u0 = ub[:heads]
        probs = softmax(base[:heads])
        weights = [probs]
        for j in range(tangents):
            ds = base[(1 + j) * heads : (2 + j) * heads] + dot_t(u0, normed[1 + j, at, :]) * factor
            weights.append(probs * (ds - jnp.sum(probs * ds, -1, keepdims=True)))
        m = dot(jnp.concatenate(weights, 0).astype(BF16), normed[0, at, :])
        low = probs.astype(BF16)
        parts = [m[:heads]]
        for j in range(tangents):
            parts.append(m[(1 + j) * heads : (2 + j) * heads] + dot(low, normed[1 + j, at, :]))
        sums += parts
    return jnp.concatenate(sums, 0).astype(BF16)


def order(sizes, heads, flip):
    micro, toks, width, hd, tangents = sizes
    streams = 1 + tangents
    share = heads // 4
    few, many = micro * streams * heads, heads * BLOCK
    shape = (many, few) if flip else (few, many)
    r = lax.broadcasted_iota(jnp.int32, shape, 1 if flip else 0)
    c = lax.broadcasted_iota(jnp.int32, shape, 0 if flip else 1)
    head, i = r % heads, r // heads
    i = (i % streams) * micro + i // streams
    return (c == head * BLOCK + i).astype(F32).astype(BF16)


def lowered(extra, micro, rows):
    width = extra[0].shape[-1]
    parts = [jnp.zeros((micro, width), F32)] + [e[:micro] for e in extra]
    used = micro * len(parts)
    return jnp.concatenate(parts + [jnp.zeros((rows - used, width), F32)], 0)


def kernel(
    n, sizes, tokens, w_qkv, tangent_value, outs, gain, final_gain, head, mean_ref, var_ref,
    a_full, b_full, normed, proj, att, state, state_in, classes, classes_in,
    a_quarter, b_quarter, a_part, b_part, cls_all, u_out, u_all, m_out, m_all, o_out, o_all,
    send, recv, local, gate, core_sems, plane_send, plane_recv, line_send, line_recv,
):
    micro, toks, width, hd, tangents = sizes
    streams = 1 + tangents
    heads = hd // HEAD
    share = heads // 4
    part = share * HEAD
    g = Gather(n, a_full, b_full, send, recv)
    me, section = g.me, g.section
    other = 1 - section
    up, down = g.z + 1 < g.nz, g.z >= 1
    plane = Plane(g, plane_send, plane_recv)
    line = Line(g, (a_part, b_part), line_send, line_recv)

    barrier = pltpu.get_barrier_semaphore()

    def greet(target, sec):
        pl.semaphore_signal(
            barrier, inc=1, device_id={"section": sec, "dp": target}, device_id_type=MESH
        )

    for near in (g.x_near, g.y_near, g.diagonal):
        greet(near, section)
    greet(me, other)
    pl.when(up)(lambda: greet(me + 4, section))
    pl.when(down)(lambda: greet(me - 4, section))

    def met():
        if g.nz > 1:
            middle = up & down
            pl.when(middle)(lambda: pl.semaphore_wait(barrier, 6))
            pl.when(jnp.logical_not(middle))(lambda: pl.semaphore_wait(barrier, 5))
        else:
            pl.semaphore_wait(barrier, 4)

    def across(src, dst, i):
        return pltpu.make_async_remote_copy(
            src_ref=src,
            dst_ref=dst,
            send_sem=core_sems.at[2 * i],
            recv_sem=core_sems.at[2 * i + 1],
            device_id={"section": other, "dp": me},
            device_id_type=MESH,
        )

    own = pl.ds(pl.multiple_of(me * g.rows, g.rows), g.rows)

    def moved(pairs):
        moves = [pltpu.make_async_copy(src, dst, local.at[i]) for i, (src, dst) in enumerate(pairs)]
        for move in moves:
            move.start()
        for move in moves:
            move.wait()

    met()

    @pl.when(section == 0)
    def _():
        pairs = [(w_qkv, a_full.at[own, pl.ds(0, 3 * hd)])]
        for j in range(tangents):
            pairs.append((tangent_value.at[j], a_full.at[own, pl.ds((3 + j) * hd, hd)]))
        pairs.append((outs, b_full.at[:, own, :]))
        moved(pairs)
        steps = [(group, d) for group in range(2) for d in range(g.nz)]
        lag = 2
        chunks = [
            lambda: (g.rest(0), first_qkv(sizes, a_full, normed, proj)),
            *[functools.partial(first_attend, sizes, proj, att, b) for b in range(micro)],
        ]
        for i in range(len(steps) + lag):
            if i < len(steps):
                g.direct(*steps[i])
            if i == 0:
                first_norm(sizes, tokens, gain, normed)
            if i == 0:
                pl.semaphore_signal(
                    gate, inc=1, device_id={"section": other, "dp": me}, device_id_type=MESH
                )
            if i >= lag:
                g.relay(*steps[i - lag])
            if i >= len(steps) - 1 and i < len(steps) + lag - 1 and chunks:
                chunks.pop(0)()
        for chunk in chunks:
            chunk()
        g.rest(1)
        first_out(sizes, tokens, b_full, att, state)
        onward = across(state, state_in, 0)
        onward.start()
        g.drain()
        onward.wait_send()
        across(classes, classes_in, 1).wait_recv()

    @pl.when(section == 1)
    def _():
        pairs = []
        for p in range(4):
            for m in range(3):
                pairs.append(
                    (w_qkv.at[:, pl.ds(m * hd + p * part, part)], a_quarter.at[p, :, pl.ds(m * part, part)])
                )
            for j in range(tangents):
                pairs.append(
                    (
                        tangent_value.at[j, :, pl.ds(p * part, part)],
                        a_quarter.at[p, :, pl.ds((3 + j) * part, part)],
                    )
                )
            pairs.append((outs.at[:, :, pl.ds(p * part, part)], b_quarter.at[p]))
        moved(pairs)

        def at_place(place):
            row = (g.z * 4 + place) * g.rows
            return pl.ds(pl.multiple_of(row, g.rows), g.rows)

        stages = [
            (0, lambda p: a_quarter.at[p], lambda p: a_part.at[at_place(p), :]),
            (1, lambda p: b_quarter.at[p], lambda p: b_part.at[:, at_place(p), :]),
            (2, lambda p: cls_all.at[plane.place], lambda p: cls_all.at[p]),
            (3, lambda p: u_out.at[p], lambda p: u_all.at[p]),
            (4, lambda p: m_out.at[p], lambda p: m_all.at[p]),
            (5, lambda p: o_out.at[p], lambda p: o_all.at[p]),
        ]
        for stage in stages[:2]:
            plane.exchange(*stage)
        moved(
            [
                (a_quarter.at[plane.place], a_part.at[own, :]),
                (b_quarter.at[plane.place], b_part.at[:, own, :]),
            ]
        )
        for stage in stages[:2]:
            plane.arrive(*stage)
        pl.semaphore_wait(gate, 1)
        line.run(0)
        line.run(1)

        across(state, state_in, 0).wait_recv()
        resid, firsts = class_rows(sizes, gain, state_in)
        cls_all[plane.place] = firsts
        plane.exchange(*stages[2])
        last_norm(sizes, gain, state_in, normed)
        plane.arrive(*stages[2])
        rows = jnp.concatenate([cls_all[k] for k in range(4)], 0)
        q = dot(rows, a_part[:, pl.ds(0, part)]).astype(BF16)
        owner = lax.broadcasted_iota(jnp.int32, (BLOCK, part), 1) // HEAD
        zero = jnp.zeros((BLOCK, part), F32)
        spread = []
        for k in range(4):
            block = q[k * BLOCK : (k + 1) * BLOCK].astype(F32)
            spread += [jnp.where(owner == h, block, zero) for h in range(share)]
        u = dot_t(jnp.concatenate(spread, 0).astype(BF16), a_part[:, pl.ds(part, part)]).astype(BF16)
        tall = share * BLOCK
        for k in range(4):
            u_out[k] = u[k * tall : (k + 1) * tall]
        plane.exchange(*stages[3])
        u_all[plane.place] = u_out[plane.place]
        plane.arrive(*stages[3])
        u48 = dot(order(sizes, heads, False), jnp.concatenate([u_all[k] for k in range(4)], 0))
        sums = last_attend(sizes, heads, u48, normed)
        spreadm = dot(order(sizes, heads, True), sums).astype(BF16)
        for k in range(4):
            m_out[k] = spreadm[k * tall : (k + 1) * tall]
        plane.exchange(*stages[4])
        m_all[plane.place] = m_out[plane.place]
        plane.arrive(*stages[4])
        m = jnp.concatenate([m_all[k] for k in range(4)], 0)
        r = [dot(m, a_part[:, pl.ds((2 + c) * part, part)]) for c in range(streams)]

        def picked(x, k):
            chosen = zero
            for h in range(share):
                at = k * tall + h * BLOCK
                chosen = jnp.where(owner == h, x[at : at + BLOCK], chosen)
            return chosen

        attended = jnp.concatenate(
            [
                picked(r[0], k) + lowered([picked(x, k) for x in r[1:]], micro, BLOCK)
                for k in range(4)
            ],
            0,
        ).astype(BF16)
        out = [dot_t(attended, b_part[c]) for c in range(streams)]
        some = o_out.shape[1]
        for k in range(4):
            at = k * BLOCK
            extra = [x[at : at + micro] for x in out[1:]]
            o_out[k] = out[0][at : at + some] + lowered(extra, micro, some)
        plane.exchange(*stages[5])
        o_all[plane.place] = o_out[plane.place]
        plane.arrive(*stages[5])
        total = o_all[0] + o_all[1] + o_all[2] + o_all[3]
        final = (resid[:some] + total).astype(BF16).astype(F32)
        classes[...] = final
        back = across(classes, classes_in, 1)
        back.start()
        classes_in[...] = final
        for stage in stages:
            plane.finish(*stage)
        line.drain(0)
        line.drain(1)
        back.wait_send()

    rows = classes_in[...]
    count = classes_in.shape[0]
    primal = jnp.concatenate([rows[:micro]] * (1 + tangents) + [rows[(1 + tangents) * micro :]], 0)
    centred, inverse, y = norm_rows(primal, final_gain[...])
    dy = norm_tangent(rows, centred, inverse, final_gain[...])
    which = lax.broadcasted_iota(jnp.int32, (count, width), 0)
    logits = dot_t(jnp.where(which < micro, y, dy).astype(BF16), head[...])
    mean_ref[:, 0, :] = logits[:micro]
    var_ref[:, 0, :] = sum(
        logits[(1 + j) * micro : (2 + j) * micro] * logits[(1 + j) * micro : (2 + j) * micro]
        for j in range(tangents)
    )


def two_sections(n):
    def shards(tokens, w_qkv, w_output, tangent_value, tangent_output, layer_gain, final_gain, head):
        micro, _, toks, width = tokens.shape
        tangents = tangent_value.shape[1]
        hd = w_output.shape[1]
        classes = head.shape[1]
        rows = width // n
        outs = jnp.swapaxes(jnp.concatenate([w_output, tangent_output[0]], 0), 1, 2)
        sizes = (micro, toks, width, hd, tangents)
        vmem = pl.BlockSpec(memory_space=pltpu.VMEM)
        anywhere = pl.BlockSpec(memory_space=pl.ANY)
        streams = 1 + tangents
        padded = -(-micro * streams // 8) * 8
        all_rows = streams * micro * toks
        tall = hd // HEAD // 4 * BLOCK
        mean, var = pl.pallas_call(
            functools.partial(kernel, n, sizes),
            out_shape=[jax.ShapeDtypeStruct((micro, 1, classes), F32)] * 2,
            in_specs=[vmem, anywhere, anywhere, anywhere, vmem, vmem, vmem],
            out_specs=[vmem, vmem],
            scratch_shapes=[
                pltpu.VMEM((width, (3 + tangents) * hd), BF16),
                pltpu.VMEM((streams, width, hd), BF16),
                pltpu.VMEM((streams, micro * toks, width), BF16),
                pltpu.VMEM((micro * toks, (3 + tangents) * hd), BF16),
                pltpu.VMEM((all_rows, hd), BF16),
                pltpu.VMEM((all_rows, width), BF16),
                pltpu.VMEM((all_rows, width), BF16),
                pltpu.VMEM((padded, width), F32),
                pltpu.VMEM((padded, width), F32),
                pltpu.VMEM((4, rows, (3 + tangents) * hd // 4), BF16),
                pltpu.VMEM((4, streams, rows, hd // 4), BF16),
                pltpu.VMEM((width, (3 + tangents) * hd // 4), BF16),
                pltpu.VMEM((streams, width, hd // 4), BF16),
                pltpu.VMEM((4, BLOCK, width), BF16),
                pltpu.VMEM((4, tall, width), BF16),
                pltpu.VMEM((4, tall, width), BF16),
                pltpu.VMEM((4, tall, width), BF16),
                pltpu.VMEM((4, tall, width), BF16),
                pltpu.VMEM((4, padded, width), F32),
                pltpu.VMEM((4, padded, width), F32),
                pltpu.SemaphoreType.DMA((send_slots(n),)),
                pltpu.SemaphoreType.DMA((n, 4)),
                pltpu.SemaphoreType.DMA((4 * (4 + tangents),)),
                pltpu.SemaphoreType.REGULAR,
                pltpu.SemaphoreType.DMA((4,)),
                pltpu.SemaphoreType.DMA((6, 3)),
                pltpu.SemaphoreType.DMA((6, 4)),
                pltpu.SemaphoreType.DMA((n // 4, 4)),
                pltpu.SemaphoreType.DMA((n // 4, 2)),
            ],
            compiler_params=pltpu.CompilerParams(
                collective_id=0, has_side_effects=True, vmem_limit_bytes=60 * 2**20
            ),
        )(
            tokens.reshape(micro, toks, width),
            w_qkv[0],
            tangent_value[0],
            outs,
            layer_gain,
            final_gain[None],
            head.T,
        )
        return mean, var

    return shards


def solution(mesh):
    n = mesh.shape["dp"]
    fast = mesh.shape["section"] == 2 and n % 4 == 0
    return jax.shard_map(
        two_sections(n) if fast else relay_shards,
        mesh=mesh,
        in_specs=(
            P(None, "dp", None, None),
            P("section", "dp", None),
            P("section", None, "dp"),
            P("section", None, "dp", None),
            P("section", None, None, "dp"),
            P("section", None),
            P(),
            P(None, "section"),
        ),
        out_specs=(P(None, "dp", "section"), P(None, "dp", "section")),
        check_vma=False,
    )
```
